128 devices in a mesh: lat: 16 (over z_hi, x, core), lon: 8 (over z_lo, y).
Axes of the slice: x: 4, y: 4, z: 4 (z_hi: 2, z_lo: 2; z = z_hi * 2 + z_lo), core: 2. Of those that a mesh axis runs over, the one named last changes fastest.
Arguments:
- ocean_state: bfloat16 [1, 192, 640, 768], P(None, 'lat', None, 'lon'), may hold values from -6 to 6
- zonal_kernel: bfloat16 [2, 5, 256, 640], replicated, may hold values from -0.15625 to 0.15625
- norm_gain: bfloat16 [2, 640], replicated, may hold values from 0.099609375 to 1.8984375
- input_weight: bfloat16 [2, 640, 1280], replicated, may hold values from -0.25 to 0.25
- output_weight: bfloat16 [2, 1280, 640], replicated, may hold values from -0.15625 to 0.15625
Outputs:
- state_out: bfloat16 [1, 192, 640, 768], P(None, 'lat', None, 'lon')
The draws below stay inside these ranges and needn't reach their ends.
All inputs are finite; a program needn't handle non-finite values.
Results may differ from the reference program's by a relative error of at most 0.009.
Values may be sent and summed in bfloat16 or wider, within the bound.
A program may use at most 128 MiB of HBM per device.

```python
import math
import jax
import jax.numpy as jnp
from jax import lax

C = 640
FF = 1280
W = 768
TAPS = 256
KROWS = 5
BLOCKS = 2
BATCH = 1
H = 192


def levels(stream_key, extent, pieces, low, largest):
    factor_of = 1.0
    for axis_at, parts in pieces:
        steps = jax.random.uniform(jax.random.fold_in(jax.random.fold_in(stream_key, 6), axis_at), (parts,), jnp.float32, low / len(pieces), largest / len(pieces))
        factor_of = factor_of * jnp.repeat(jnp.exp(steps), extent[axis_at] // parts).reshape((-1,) + (1,) * (len(extent) - 1 - axis_at))
    return factor_of


def gaussian(own_key, shape, spread, most, cuts=(), kind=jnp.bfloat16):
    result = spread * jax.random.normal(own_key, shape, jnp.float32)
    if cuts:
        result = result * levels(own_key, shape, cuts, -0.22, 0.18)
    return jnp.clip(result, -most, most).astype(kind)


def setup_inputs(seed: int = 0) -> dict:
    seeds = jax.random.split(jax.random.key(seed), 6)
    ocean_state = gaussian(seeds[0], (BATCH, H, C, W), 1.0, 6.0, ((1, 16), (3, 8)))
    zonal_kernel = gaussian(seeds[1], (BLOCKS, KROWS, TAPS, C), (KROWS * TAPS) ** -0.5, 0.15625)
    norm_gain = jnp.clip(1.0 + 0.18 * jax.random.normal(seeds[2], (BLOCKS, C), jnp.float32), 0.099609375, 1.8984375).astype(jnp.bfloat16)
    input_weight = gaussian(seeds[3], (BLOCKS, C, FF), C ** -0.5, 0.25)
    output_weight = gaussian(seeds[4], (BLOCKS, FF, C), FF ** -0.5, 0.15625)
    return dict(ocean_state=ocean_state, zonal_kernel=zonal_kernel, norm_gain=norm_gain, input_weight=input_weight, output_weight=output_weight)


def latitude_weights(row_start, row_count, total_rows):
    row_index = row_start + jnp.arange(row_count, dtype=jnp.int32)
    return jnp.sin(jnp.pi * (row_index.astype(jnp.float32) + 0.5) / total_rows)

def zonal_mix(current, kernel_layer):
    weights = latitude_weights(0, H, H)
    group_size = math.gcd(C, 64)
    group_count = C // group_size
    weighted = current.astype(jnp.float32) * weights[None, :, None, None]
    weighted = weighted.reshape(BATCH, H, group_count, group_size, W).transpose(2, 0, 1, 3, 4)
    tap_values = kernel_layer.astype(jnp.float32).reshape(KROWS, TAPS, group_count, group_size).transpose(2, 0, 3, 1)
    rim_rows = KROWS // 2

    def per_group(group_pair):
        signal_rows, filters = group_pair
        filters = jnp.pad(filters, ((0, 0), (0, 0), (0, W - TAPS)))
        filters = jnp.roll(filters, -(TAPS // 2), axis=2)
        spectra = jnp.fft.rfft(filters, axis=2)
        signal = jnp.fft.rfft(signal_rows, axis=3)
        padded = jnp.pad(signal, ((0, 0), (rim_rows, rim_rows), (0, 0), (0, 0)))
        summed = padded[:, 0:H] * spectra[0]
        for offset in range(1, KROWS):
            summed = summed + padded[:, offset:offset + H] * spectra[offset]
        return jnp.fft.irfft(summed, n=W, axis=3)
    mapped = lax.map(per_group, (weighted, tap_values))
    return mapped.transpose(1, 2, 0, 3, 4).reshape(BATCH, H, C, W)

def feed_forward(mixed_in, gain_layer, input_layer, output_layer):
    gain_values = gain_layer.astype(jnp.float32)
    lifting = input_layer.astype(jnp.float32)
    lowered = output_layer.astype(jnp.float32)

    def per_row(lat_slab):
        values = lat_slab.astype(jnp.float32)
        average = lax.optimization_barrier(jnp.mean(values, axis=1, keepdims=True))
        variance = lax.optimization_barrier(jnp.mean(jnp.square(values - average), axis=1, keepdims=True))
        normed = ((values - average) * lax.rsqrt(variance + 1e-05) * gain_values[None, :, None]).astype(jnp.bfloat16)
        hidden = jnp.einsum('bcw,cf->bwf', normed.astype(jnp.float32), lifting)
        hidden = jax.nn.gelu(hidden, approximate=False).astype(jnp.bfloat16)
        projected = jnp.einsum('bwf,fc->bcw', hidden.astype(jnp.float32), lowered)
        return (values + projected).astype(jnp.bfloat16)
    rows_first = mixed_in.transpose(1, 0, 2, 3)
    return lax.map(per_row, rows_first).transpose(1, 0, 2, 3)

def reference(ocean_state, zonal_kernel, norm_gain, input_weight, output_weight):
    current = ocean_state
    for layer_index in range(BLOCKS):
        convolved = zonal_mix(current, zonal_kernel[layer_index])
        mixed_out = (current.astype(jnp.float32) + jax.nn.gelu(convolved, approximate=False)).astype(jnp.bfloat16)
        current = feed_forward(mixed_out, norm_gain[layer_index], input_weight[layer_index], output_weight[layer_index])
    return current
```

```python
import functools

import numpy as np
import jax
import jax.numpy as jnp
from jax import lax
from jax.experimental import pallas as pl
from jax.experimental.pallas import tpu as pltpu
from jax.sharding import PartitionSpec as P

C = 640
FF = 1280
W = 768
TAPS = 256
KROWS = 5
BLOCKS = 2
LON = 8
ROWS = 12
SHARE = C // LON
COLS = W // LON
HALF = W // 2
GROUPS = 3
TILES = 9
MESH = pl.DeviceIdType.MESH
F32 = jnp.float32
BF16 = jnp.bfloat16


def unit_place(unit):
    device, third = divmod(unit, 3)
    half, quarter = divmod(device, 4)
    return ((2 * third + half) * 4 + quarter) * 32


def basis():
    w = np.arange(W)[:, None]
    f = np.arange(HALF)[None, :]
    angle = 2.0 * np.pi / W * ((w * f) % W)
    sine = np.where(f == 0, 1.0 - 2.0 * (w % 2), np.sin(angle))
    full = np.concatenate([np.cos(angle), sine], axis=1)
    placed = np.zeros_like(full)
    for unit in range(W // 32):
        at = unit_place(unit)
        placed[at : at + 32] = full[32 * unit : 32 * unit + 32]
    return placed


def row_weights(total):
    h = np.arange(total)
    quad = np.sin(np.pi * (h + 0.5) / total)
    return np.concatenate([np.zeros(2), quad, np.zeros(2)]).astype(np.float32)


def nt(a, b):
    return lax.dot_general(a, b, (((1,), (1,)), ((), ())), preferred_element_type=F32)


def nn(a, b):
    return lax.dot_general(a, b, (((1,), (0,)), ((), ())), preferred_element_type=F32)


def gelu(x):
    return 0.5 * x * (1.0 + lax.erf(x * 0.7071067811865476))


def swap4(tiles):
    v0, v1, v2, v3 = [t.astype(F32) for t in tiles]
    lane = lax.broadcasted_iota(jnp.int32, v0.shape, 1)
    low = lane < 64
    even = (lane & 32) == 0
    roll = lambda v, s: pltpu.roll(v, s, 1)
    u0 = jnp.where(low, v0, roll(v2, 64))
    u2 = jnp.where(low, roll(v0, 64), v2)
    u1 = jnp.where(low, v1, roll(v3, 64))
    u3 = jnp.where(low, roll(v1, 64), v3)
    outs = (
        jnp.where(even, u0, roll(u1, 32)),
        jnp.where(even, roll(u0, 96), u1),
        jnp.where(even, u2, roll(u3, 32)),
        jnp.where(even, roll(u2, 96), u3),
    )
    return [o.astype(BF16) for o in outs]


def loop(count, body):
    def step(i, carry):
        body(i)
        return carry

    lax.fori_loop(0, count, step, 0)


def kernel(
    quad_ref, gain_ref, x_hbm, kern_hbm, w1_hbm, w2_hbm, f_hbm, out_hbm,
    rows_in, xpos, r1, xr, spec, kf, yb, s2, r2, w1t, w2t, hid, nrm, gainb,
    fb, kraw, w1, w2,
    in_sem, load_sem, out_sem, a_send, a_recv, b_send, b_recv, h_send, h_recv,
):
    me = lax.axis_index("lon")
    lat = lax.axis_index("lat")
    lats = lax.axis_size("lat")
    up = lax.rem(lat + lats - 1, lats)
    down = lax.rem(lat + 1, lats)
    mine = pl.ds(pl.multiple_of(me * SHARE, SHARE), SHARE)

    def tiles_of(g):
        return pl.ds(3 * g, 3)

    def fetch(g):
        return pltpu.make_async_copy(
            x_hbm.at[0, pl.ds(4 * g, 4)], rows_in.at[pl.ds(4 * g, 4)], in_sem.at[g]
        )

    for g in range(GROUPS):
        fetch(g).start()
    loads = [
        pltpu.make_async_copy(src, dst, load_sem.at[i])
        for i, (src, dst) in enumerate(
            [(kern_hbm, kraw), (f_hbm, fb), (w1_hbm, w1), (w2_hbm, w2)]
        )
    ]
    for copy in loads:
        copy.start()

    barrier = pltpu.get_barrier_semaphore()
    for d in range(1, LON):
        pl.semaphore_signal(
            barrier, inc=1, device_id={"lon": lax.rem(me + d, LON)}, device_id_type=MESH
        )
    for other in (up, down):
        pl.semaphore_signal(barrier, inc=1, device_id={"lat": other}, device_id_type=MESH)

    def a_copy(l, g, d):
        peer = lax.rem(me + d, LON)
        theirs = pl.ds(pl.multiple_of(peer * SHARE, SHARE), SHARE)
        return pltpu.make_async_remote_copy(
            src_ref=xpos.at[l, tiles_of(g), theirs],
            dst_ref=r1.at[l, me, tiles_of(g)],
            send_sem=a_send.at[l, g, d - 1],
            recv_sem=a_recv.at[l, g, d - 1],
            device_id={"lon": peer},
            device_id_type=MESH,
        )

    def b_copy(l, g, d):
        peer = lax.rem(me + d, LON)
        return pltpu.make_async_remote_copy(
            src_ref=s2.at[l, peer, tiles_of(g)],
            dst_ref=r2.at[l, tiles_of(g), mine],
            send_sem=b_send.at[l, g, d - 1],
            recv_sem=b_recv.at[l, g, d - 1],
            device_id={"lon": peer},
            device_id_type=MESH,
        )

    def halo_copy(l, side):
        src, dst, other = ((2, 14, up), (12, 0, down))[side]
        return pltpu.make_async_remote_copy(
            src_ref=xr.at[l, pl.ds(src, 2)],
            dst_ref=xr.at[l, pl.ds(dst, 2)],
            send_sem=h_send.at[l, side],
            recv_sem=h_recv.at[l, side],
            device_id={"lat": other},
            device_id_type=MESH,
        )

    def start_a(l, g):
        for d in range(1, LON):
            a_copy(l, g, d).start()
        r1[l, me, tiles_of(g)] = xpos[l, tiles_of(g), mine]

    def pack_input(g):
        def piece(i):
            rows = pl.ds(pl.multiple_of(i * SHARE, SHARE), SHARE)
            pad = jnp.zeros((SHARE, 128 - COLS), BF16)
            tiles = [
                jnp.concatenate([rows_in[4 * g + r, rows, :], pad], axis=1) for r in range(4)
            ]
            packed = swap4(tiles)
            for third in range(3):
                xpos[0, 3 * g + third, rows, :] = packed[third]

        loop(C // SHARE, piece)

    for g in range(GROUPS):
        fetch(g).wait()
        pack_input(g)
        if g == 0:
            pl.semaphore_wait(barrier, LON + 1)
        start_a(0, g)

    loads[0].wait()
    loads[1].wait()
    taps_basis = [unit_place((32 * u - TAPS // 2) % W // 32) for u in range(TAPS // 32)]

    def spectra(i):
        l = i // KROWS
        r = lax.rem(i, KROWS)
        pick = (
            lax.broadcasted_iota(jnp.int32, (SHARE, C), 1)
            == lax.broadcasted_iota(jnp.int32, (SHARE, C), 0) + me * SHARE
        ).astype(BF16)
        taps = nt(pick, kraw[l, r]).astype(BF16)
        tap_rows = jnp.concatenate([fb[p : p + 32, :] for p in taps_basis], axis=0)
        full = nn(taps, tap_rows)
        keep = lax.broadcasted_iota(jnp.int32, (SHARE, HALF), 1) >= 1
        scale = jnp.where(keep, 2.0 / W, 1.0 / W).astype(F32)
        real = full[:, :HALF] * scale
        sine = full[:, HALF:] * scale
        kf[l, r, 0] = real
        kf[l, r, 1] = jnp.where(keep, sine, 0.0)
        kf[l, r, 2] = jnp.where(keep, real, sine)

    loop(BLOCKS * KROWS, spectra)
    loads[2].wait()
    loads[3].wait()

    def unit_matrix(n):
        return (
            lax.broadcasted_iota(jnp.int32, (n, n), 0)
            == lax.broadcasted_iota(jnp.int32, (n, n), 1)
        ).astype(BF16)

    for l in range(BLOCKS):

        def turn1(i):
            at = pl.ds(pl.multiple_of(i * 256, 256), 256)
            w1t[l, at, :] = nt(unit_matrix(256), w1[l, :, at]).astype(BF16)

        def turn2(i):
            at = pl.ds(pl.multiple_of(i * 128, 128), 128)
            w2t[l, at, :] = nt(unit_matrix(128), w2[l, :, at]).astype(BF16)
            row = jnp.broadcast_to(gain_ref[pl.ds(l, 1), at].astype(F32), (128, 128))
            gainb[l, at, :] = row.T

        loop(FF // 256, turn1)
        loop(C // 128, turn2)

    def unpack(l, g):
        def piece(third):
            for half in range(2):
                tiles = [r1[l, 4 * half + q, 3 * g + third] for q in range(4)]
                rows = swap4(tiles)
                at = pl.ds(pl.multiple_of(256 * third, 128) + 128 * half, 128)
                for r in range(4):
                    xr[l, 2 + 4 * g + r, :, at] = rows[r]

        loop(3, piece)

    def transform(l, first, count):
        def piece(n):
            at = pl.ds(pl.multiple_of(n * 256, 256), 256)
            lhs = xr[l, pl.ds(first, count)].reshape(count * SHARE, W)
            part = nn(lhs, fb[:, at])
            for r in range(count):
                weight = quad_ref[lat * ROWS + first + r]
                spec[first + r, :, at] = part[SHARE * r : SHARE * (r + 1)] * weight

        loop(3, piece)

    def convolve(l, g):
        def bands(i):
            rows = pl.ds(pl.multiple_of(i * 16, 16), 16)
            for n in range(3):
                re_at = pl.ds(128 * n, 128)
                im_at = pl.ds(HALF + 128 * n, 128)
                factors = [
                    [kf[l, r, j, rows, re_at] for j in range(3)] for r in range(KROWS)
                ]
                for row in range(4):
                    real = sine = None
                    for r in range(KROWS):
                        a = spec[4 * g + row + r, rows, re_at]
                        b = spec[4 * g + row + r, rows, im_at]
                        kr, kc, ks = factors[r]
                        new_real = a * kr - b * kc
                        new_sine = a * kc + b * ks
                        real = new_real if real is None else real + new_real
                        sine = new_sine if sine is None else sine + new_sine
                    yb[row, rows, re_at] = real.astype(BF16)
                    yb[row, rows, im_at] = sine.astype(BF16)

        loop(SHARE // 16, bands)

        def invert(third):
            at = pl.multiple_of(256 * third, 256)
            lhs = yb[...].reshape(4 * SHARE, W)
            part = nt(lhs, fb[pl.ds(at, 256), :])
            for half in range(2):
                tiles = []
                for r in range(4):
                    conv = part[SHARE * r : SHARE * (r + 1), 128 * half : 128 * (half + 1)]
                    old = xr[l, 2 + 4 * g + r, :, pl.ds(at + 128 * half, 128)]
                    tiles.append((old.astype(F32) + gelu(conv)).astype(BF16))
                packed = swap4(tiles)
                for q in range(4):
                    s2[l, 4 * half + q, 3 * g + third] = packed[q]

        loop(3, invert)

    def start_b(l, g):
        for d in range(1, LON):
            b_copy(l, g, d).start()
        r2[l, tiles_of(g), mine] = s2[l, me, tiles_of(g)]

    def feed_forward(l, g):
        def norm(t):
            values = r2[l, 3 * g + t].astype(F32)
            average = jnp.sum(values, axis=0, keepdims=True) * (1.0 / C)
            centred = values - average
            variance = jnp.sum(centred * centred, axis=0, keepdims=True) * (1.0 / C)
            scaled = centred * lax.rsqrt(variance + 1e-05) * gainb[l]
            nrm[:, pl.ds(pl.multiple_of(128 * t, 128), 128)] = scaled.astype(BF16)

        loop(3, norm)

        def first(i):
            at = pl.ds(pl.multiple_of(i * 256, 256), 256)
            hid[at, :] = gelu(nn(w1t[l, at, :], nrm[...])).astype(BF16)

        loop(FF // 256, first)

        def second(i):
            at = pl.ds(pl.multiple_of(i * 128, 128), 128)
            out = nn(w2t[l, at, :], hid[...])
            for t in range(3):
                old = r2[l, 3 * g + t, at, :].astype(F32)
                new = (old + out[:, 128 * t : 128 * (t + 1)]).astype(BF16)
                xpos[(l + 1) % 2, 3 * g + t, at, :] = new

        loop(C // 128, second)

    def finish(g):
        def piece(i):
            rows = pl.ds(pl.multiple_of(i * SHARE, SHARE), SHARE)
            tiles = [xpos[0, 3 * g + t, rows, :] for t in (0, 1, 2, 2)]
            apart = swap4(tiles)
            for r in range(4):
                rows_in[4 * g + r, rows, :] = apart[r][:, :COLS]

        loop(C // SHARE, piece)

    def store(g):
        return pltpu.make_async_copy(
            rows_in.at[pl.ds(4 * g, 4)], out_hbm.at[0, pl.ds(4 * g, 4)], out_sem.at[g]
        )

    order = (1, 0, 2)
    for l in range(BLOCKS):
        for g in (0, 1, 2) if l == 0 else order:
            for d in range(1, LON):
                a_copy(l, g, d).wait_recv()
            unpack(l, g)
            if g == 0:
                halo_copy(l, 0).start()
            if g == 2:
                halo_copy(l, 1).start()
            transform(l, 2 + 4 * g, 4)
        if l == 1:
            pass
        for g in order:
            if g == 0:
                halo_copy(l, 1).wait_recv()
                transform(l, 0, 2)
            if g == 2:
                halo_copy(l, 0).wait_recv()
                transform(l, 14, 2)
            convolve(l, g)
            start_b(l, g)
        if l == 1:
            pass
        if l == 0:
            pass
        for g in order:
            for d in range(1, LON):
                b_copy(l, g, d).wait_recv()
            if l == 1:
                for d in range(1, LON):
                    a_copy(0, g, d).wait_send()
            feed_forward(l, g)
            if l == 0:
                start_a(1, g)
            else:
                finish(g)
                store(g).start()
    for g in range(GROUPS):
        for d in range(1, LON):
            a_copy(1, g, d).wait_send()
            b_copy(0, g, d).wait_send()
            b_copy(1, g, d).wait_send()
        store(g).wait()
    for l in range(BLOCKS):
        for side in range(2):
            halo_copy(l, side).wait_send()


def body(ocean_state, zonal_kernel, norm_gain, input_weight, output_weight):
    total = ROWS * lax.axis_size("lat")
    quad = jnp.asarray(row_weights(total))
    table = jnp.asarray(basis().astype(jnp.bfloat16))
    hbm = pl.BlockSpec(memory_space=pl.ANY)
    return pl.pallas_call(
        kernel,
        out_shape=jax.ShapeDtypeStruct((1, ROWS, C, COLS), BF16),
        in_specs=[
            pl.BlockSpec(memory_space=pltpu.SMEM),
            pl.BlockSpec(memory_space=pltpu.VMEM),
            hbm, hbm, hbm, hbm, hbm,
        ],
        out_specs=hbm,
        scratch_shapes=[
            pltpu.VMEM((ROWS, C, COLS), BF16),
            pltpu.VMEM((2, TILES, C, 128), BF16),
            pltpu.VMEM((2, LON, TILES, SHARE, 128), BF16),
            pltpu.VMEM((2, ROWS + 4, SHARE, W), BF16),
            pltpu.VMEM((ROWS + 4, SHARE, W), F32),
            pltpu.VMEM((2, KROWS, 3, SHARE, HALF), F32),
            pltpu.VMEM((4, SHARE, W), BF16),
            pltpu.VMEM((2, LON, TILES, SHARE, 128), BF16),
            pltpu.VMEM((2, TILES, C, 128), BF16),
            pltpu.VMEM((2, FF, C), BF16),
            pltpu.VMEM((2, C, FF), BF16),
            pltpu.VMEM((FF, 384), BF16),
            pltpu.VMEM((C, 384), BF16),
            pltpu.VMEM((2, C, 128), F32),
            pltpu.VMEM((W, W), BF16),
            pltpu.VMEM((BLOCKS, KROWS, TAPS, C), BF16),
            pltpu.VMEM((BLOCKS, C, FF), BF16),
            pltpu.VMEM((BLOCKS, FF, C), BF16),
            pltpu.SemaphoreType.DMA((GROUPS,)),
            pltpu.SemaphoreType.DMA((4,)),
            pltpu.SemaphoreType.DMA((GROUPS,)),
            pltpu.SemaphoreType.DMA((2, GROUPS, LON - 1)),
            pltpu.SemaphoreType.DMA((2, GROUPS, LON - 1)),
            pltpu.SemaphoreType.DMA((2, GROUPS, LON - 1)),
            pltpu.SemaphoreType.DMA((2, GROUPS, LON - 1)),
            pltpu.SemaphoreType.DMA((2, 2)),
            pltpu.SemaphoreType.DMA((2, 2)),
        ],
        compiler_params=pltpu.CompilerParams(
            collective_id=0, has_side_effects=True, vmem_limit_bytes=62 * 1024 * 1024
        ),
    )(quad, norm_gain, ocean_state, zonal_kernel, input_weight, output_weight, table)


def solution(mesh):
    in_specs = (P(None, "lat", None, "lon"), P(), P(), P(), P())
    out_specs = P(None, "lat", None, "lon")
    return jax.shard_map(body, mesh=mesh, in_specs=in_specs, out_specs=out_specs, check_vma=False)
```

```python
import functools

import numpy as np
import jax
import jax.numpy as jnp
from jax import lax
from jax.experimental import pallas as pl
from jax.experimental.pallas import tpu as pltpu
from jax.sharding import PartitionSpec as P

C = 640
FF = 1280
W = 768
TAPS = 256
KROWS = 5
BLOCKS = 2
LON = 8
ROWS = 12
SHARE = C // LON
COLS = W // LON
HALF = W // 2
GROUPS = 3
SPLIT = 32
A_ORDER = ((0, 1, 2), (1, 2, 0))
B_ORDER = ((1, 2, 0), (1, 0, 2))
TILES = 9
MESH = pl.DeviceIdType.MESH
F32 = jnp.float32
BF16 = jnp.bfloat16


def unit_place(unit):
    device, third = divmod(unit, 3)
    half, quarter = divmod(device, 4)
    return ((2 * third + half) * 4 + quarter) * 32


def basis():
    w = np.arange(W)[:, None]
    f = np.arange(HALF)[None, :]
    angle = 2.0 * np.pi / W * ((w * f) % W)
    sine = np.where(f == 0, 1.0 - 2.0 * (w % 2), np.sin(angle))
    full = np.concatenate([np.cos(angle), sine], axis=1)
    placed = np.zeros_like(full)
    for unit in range(W // 32):
        at = unit_place(unit)
        placed[at : at + 32] = full[32 * unit : 32 * unit + 32]
    return placed


def row_weights(total):
    h = np.arange(total)
    quad = np.sin(np.pi * (h + 0.5) / total)
    return np.concatenate([np.zeros(2), quad, np.zeros(2)]).astype(np.float32)


def nt(a, b):
    return lax.dot_general(a, b, (((1,), (1,)), ((), ())), preferred_element_type=F32)


def nn(a, b):
    return lax.dot_general(a, b, (((1,), (0,)), ((), ())), preferred_element_type=F32)


def gelu(x):
    return 0.5 * x * (1.0 + lax.erf(x * 0.7071067811865476))


def swap4(tiles):
    v0, v1, v2, v3 = tiles
    lane = lax.broadcasted_iota(jnp.int32, v0.shape, 1)
    low = lane < 64
    even = (lane & 32) == 0
    roll = lambda v, s: pltpu.roll(v, s, 1)
    u0 = jnp.where(low, v0, roll(v2, 64))
    u2 = jnp.where(low, roll(v0, 64), v2)
    u1 = jnp.where(low, v1, roll(v3, 64))
    u3 = jnp.where(low, roll(v1, 64), v3)
    return (
        jnp.where(even, u0, roll(u1, 32)),
        jnp.where(even, roll(u0, 96), u1),
        jnp.where(even, u2, roll(u3, 32)),
        jnp.where(even, roll(u2, 96), u3),
    )


def loop(count, body):
    def step(i, carry):
        body(i)
        return carry

    lax.fori_loop(0, count, step, 0)


def kernel(
    quad_ref, gain_ref, x_hbm, kern_hbm, w1_hbm, w2_hbm, f_hbm, out_hbm,
    rows_in, xpos, r1, xr, spec, kf, yb, s2, r2, w1t, w2t, hid, nrm, gainb,
    fb, fbt, kraw, w1, w2,
    in_sem, load_sem, out_sem, a_send, a_recv, b_send, b_recv, h_send, h_recv,
):
    me = lax.axis_index("lon")
    lat = lax.axis_index("lat")
    lats = lax.axis_size("lat")
    up = lax.rem(lat + lats - 1, lats)
    down = lax.rem(lat + 1, lats)
    mine = pl.ds(pl.multiple_of(me * SHARE, SHARE), SHARE)

    def tiles_of(g):
        return pl.ds(3 * g, 3)

    def fetch(g):
        return pltpu.make_async_copy(
            x_hbm.at[0, pl.ds(4 * g, 4)], rows_in.at[pl.ds(4 * g, 4)], in_sem.at[g]
        )

    for g in range(GROUPS):
        fetch(g).start()
    loads = [
        pltpu.make_async_copy(src, dst, load_sem.at[i])
        for i, (src, dst) in enumerate(
            [(kern_hbm, kraw), (f_hbm, fb), (w1_hbm, w1), (w2_hbm, w2)]
        )
    ]
    for copy in loads:
        copy.start()

    barrier = pltpu.get_barrier_semaphore()
    for d in range(1, LON):
        pl.semaphore_signal(
            barrier, inc=1, device_id={"lon": lax.rem(me + d, LON)}, device_id_type=MESH
        )
    for other in (up, down):
        pl.semaphore_signal(barrier, inc=1, device_id={"lat": other}, device_id_type=MESH)

    def a_parts(l, g):
        if g == A_ORDER[l][2]:
            return [(2, 0, SPLIT), (3, SPLIT, SHARE - SPLIT)]
        return [(A_ORDER[l].index(g), 0, SHARE)]

    def b_parts(l, g):
        if g == B_ORDER[l][0]:
            return [(0, 0, SPLIT), (1, SPLIT, SHARE - SPLIT)]
        return [(1 + B_ORDER[l].index(g), 0, SHARE)]

    def channels(owner, first, count):
        return pl.ds(pl.multiple_of(owner * SHARE + first, 16), count)

    def a_copy(l, g, part, d):
        slot, first, count = part
        peer = lax.rem(me + d, LON)
        return pltpu.make_async_remote_copy(
            src_ref=xpos.at[l, tiles_of(g), channels(peer, first, count)],
            dst_ref=r1.at[l, me, tiles_of(g), pl.ds(first, count)],
            send_sem=a_send.at[l, slot, d - 1],
            recv_sem=a_recv.at[l, slot, d - 1],
            device_id={"lon": peer},
            device_id_type=MESH,
        )

    def b_copy(l, g, part, d):
        slot, first, count = part
        peer = lax.rem(me + d, LON)
        return pltpu.make_async_remote_copy(
            src_ref=s2.at[l, peer, tiles_of(g), pl.ds(first, count)],
            dst_ref=r2.at[l, tiles_of(g), channels(me, first, count)],
            send_sem=b_send.at[l, slot, d - 1],
            recv_sem=b_recv.at[l, slot, d - 1],
            device_id={"lon": peer},
            device_id_type=MESH,
        )

    def halo_copy(l, side):
        src, dst, other = ((2, 14, up), (12, 0, down))[side]
        return pltpu.make_async_remote_copy(
            src_ref=xr.at[l, pl.ds(src, 2)],
            dst_ref=xr.at[l, pl.ds(dst, 2)],
            send_sem=h_send.at[l, side],
            recv_sem=h_recv.at[l, side],
            device_id={"lat": other},
            device_id_type=MESH,
        )

    def start_a(l, g):
        for part in a_parts(l, g):
            for d in range(1, LON):
                a_copy(l, g, part, d).start()
        r1[l, me, tiles_of(g)] = xpos[l, tiles_of(g), mine]

    def pack_input(g):
        def piece(i):
            at = pl.ds(pl.multiple_of(i * 128, 128), 128)
            for third in range(3):
                lons = pl.ds(32 * third, 32)
                tile = jnp.concatenate([rows_in[4 * g + r, lons, at] for r in range(4)], axis=0)
                xpos[0, 3 * g + third, at, :] = tile.T

        loop(C // 128, piece)

    for g in range(GROUPS):
        fetch(g).wait()
        pack_input(g)
        if g == 0:
            pl.semaphore_wait(barrier, LON + 1)
        start_a(0, g)

    def unit_matrix(n):
        return (
            lax.broadcasted_iota(jnp.int32, (n, n), 0)
            == lax.broadcasted_iota(jnp.int32, (n, n), 1)
        ).astype(BF16)

    loads[0].wait()
    loads[1].wait()
    taps_basis = [unit_place((32 * u - TAPS // 2) % W // 32) for u in range(TAPS // 32)]

    def spectra(i):
        l = i // KROWS
        r = lax.rem(i, KROWS)
        pick = (
            lax.broadcasted_iota(jnp.int32, (SHARE, C), 1)
            == lax.broadcasted_iota(jnp.int32, (SHARE, C), 0) + me * SHARE
        ).astype(BF16)
        taps = nt(pick, kraw[l, r]).astype(BF16)
        tap_rows = jnp.concatenate([fb[p : p + 32, :] for p in taps_basis], axis=0)
        full = nn(taps, tap_rows)
        keep = lax.broadcasted_iota(jnp.int32, (SHARE, HALF), 1) >= 1
        scale = jnp.where(keep, 2.0 / W, 1.0 / W).astype(F32)
        real = full[:, :HALF] * scale
        sine = full[:, HALF:] * scale
        kf[l, r, 0] = real
        kf[l, r, 1] = jnp.where(keep, sine, 0.0)
        kf[l, r, 2] = jnp.where(keep, real, sine)

    loop(BLOCKS * KROWS, spectra)

    def turn0(i):
        at = pl.ds(pl.multiple_of(i * 256, 256), 256)
        fbt[at, :] = nt(unit_matrix(256), fb[:, at]).astype(BF16)

    loop(W // 256, turn0)
    loads[2].wait()
    loads[3].wait()

    for l in range(BLOCKS):

        def turn1(i):
            at = pl.ds(pl.multiple_of(i * 256, 256), 256)
            w1t[l, at, :] = nt(unit_matrix(256), w1[l, :, at]).astype(BF16)

        def turn2(i):
            at = pl.ds(pl.multiple_of(i * 128, 128), 128)
            w2t[l, at, :] = nt(unit_matrix(128), w2[l, :, at]).astype(BF16)
            row = jnp.broadcast_to(gain_ref[pl.ds(l, 1), at].astype(F32), (128, 128))
            gainb[l, at, :] = row.T

        loop(FF // 256, turn1)
        loop(C // 128, turn2)

    def unpack(l, g, first, count):
        some = pl.ds(first, count)

        def piece(third):
            for half in range(2):
                tiles = [r1[l, 4 * half + q, 3 * g + third, some, :] for q in range(4)]
                rows = swap4(tiles)
                at = pl.ds(pl.multiple_of(256 * third, 128) + 128 * half, 128)
                for r in range(4):
                    xr[l, 2 + 4 * g + r, some, at] = rows[r]

        loop(3, piece)

    def transform(l, top, rows, first, count):
        some = pl.ds(first, count)

        def piece(n):
            at = pl.ds(pl.multiple_of(n * 256, 256), 256)
            lhs = xr[l, pl.ds(top, rows), some, :].reshape(rows * count, W)
            part = nn(lhs, fb[:, at])
            for r in range(rows):
                weight = quad_ref[lat * ROWS + top + r]
                spec[top + r, some, at] = part[count * r : count * (r + 1)] * weight

        loop(3, piece)

    def convolve(l, g, first, count):
        some = pl.ds(first, count)

        def bands(i):
            rows = pl.ds(pl.multiple_of(first + i * 16, 16), 16)
            for n in range(3):
                re_at = pl.ds(128 * n, 128)
                im_at = pl.ds(HALF + 128 * n, 128)
                factors = [
                    [kf[l, r, j, rows, re_at] for j in range(3)] for r in range(KROWS)
                ]
                for row in range(4):
                    real = sine = None
                    for r in range(KROWS):
                        a = spec[4 * g + row + r, rows, re_at]
                        b = spec[4 * g + row + r, rows, im_at]
                        kr, kc, ks = factors[r]
                        new_real = a * kr - b * kc
                        new_sine = a * kc + b * ks
                        real = new_real if real is None else real + new_real
                        sine = new_sine if sine is None else sine + new_sine
                    yb[row, rows, re_at] = real.astype(BF16)
                    yb[row, rows, im_at] = sine.astype(BF16)

        loop(count // 16, bands)

        def invert(third):
            at = pl.multiple_of(256 * third, 256)
            lhs = yb[:, some, :].reshape(4 * count, W)
            part = nn(lhs, fbt[:, pl.ds(at, 256)])
            for half in range(2):
                tiles = []
                for r in range(4):
                    conv = part[count * r : count * (r + 1), 128 * half : 128 * (half + 1)]
                    old = xr[l, 2 + 4 * g + r, some, pl.ds(at + 128 * half, 128)]
                    tiles.append((old.astype(F32) + gelu(conv)).astype(BF16))
                packed = swap4(tiles)
                for q in range(4):
                    s2[l, 4 * half + q, 3 * g + third, some, :] = packed[q]

        loop(3, invert)

    def start_b(l, g, part):
        slot, first, count = part
        for d in range(1, LON):
            b_copy(l, g, part, d).start()
        r2[l, tiles_of(g), channels(me, first, count)] = s2[
            l, me, tiles_of(g), pl.ds(first, count)
        ]

    def feed_forward(l, g):
        def norm(t):
            values = r2[l, 3 * g + t].astype(F32)
            average = jnp.sum(values, axis=0, keepdims=True) * (1.0 / C)
            centred = values - average
            variance = jnp.sum(centred * centred, axis=0, keepdims=True) * (1.0 / C)
            scaled = centred * lax.rsqrt(variance + 1e-05) * gainb[l]
            nrm[:, pl.ds(pl.multiple_of(128 * t, 128), 128)] = scaled.astype(BF16)

        loop(3, norm)

        def first(i):
            at = pl.ds(pl.multiple_of(i * 640, 640), 640)
            hid[at, :] = gelu(nn(w1t[l, at, :], nrm[...])).astype(BF16)

        loop(FF // 640, first)
        out = nn(w2t[l], hid[...])
        for t in range(3):
            old = r2[l, 3 * g + t].astype(F32)
            new = (old + out[:, 128 * t : 128 * (t + 1)]).astype(BF16)
            if l == 0:
                xpos[1, 3 * g + t] = new
            else:
                lons = pl.ds(32 * t, 32)
                for i in range(C // 128):
                    turned = new[128 * i : 128 * (i + 1), :].T
                    for r in range(4):
                        rows_in[4 * g + r, lons, pl.ds(128 * i, 128)] = turned[
                            32 * r : 32 * (r + 1), :
                        ]

    def store(g):
        return pltpu.make_async_copy(
            rows_in.at[pl.ds(4 * g, 4)], out_hbm.at[0, pl.ds(4 * g, 4)], out_sem.at[g]
        )

    def take(l, g, part):
        for d in range(1, LON):
            a_copy(l, g, part, d).wait_recv()
        unpack(l, g, *part[1:])
        if part[1] + part[2] == SHARE and g != 1:
            halo_copy(l, g // 2).start()
        transform(l, 2 + 4 * g, 4, *part[1:])

    def give(l, g, part):
        convolve(l, g, *part[1:])
        start_b(l, g, part)

    for l in range(BLOCKS):
        for g in A_ORDER[l][:2]:
            take(l, g, a_parts(l, g)[0])
        last = A_ORDER[l][2]
        for arrived, ready in zip(a_parts(l, last), b_parts(l, 1)):
            take(l, last, arrived)
            give(l, 1, ready)
        for g in B_ORDER[l][1:]:
            halo_copy(l, 1 - g // 2).wait_recv()
            transform(l, 0 if g == 0 else ROWS + 2, 2, 0, SHARE)
            give(l, g, b_parts(l, g)[0])
        for g in B_ORDER[l]:
            for part in b_parts(l, g):
                for d in range(1, LON):
                    b_copy(l, g, part, d).wait_recv()
            feed_forward(l, g)
            if l == 0:
                start_a(1, g)
            else:
                store(g).start()
    for l in range(BLOCKS):
        for g in range(GROUPS):
            for d in range(1, LON):
                for part in a_parts(l, g):
                    a_copy(l, g, part, d).wait_send()
                for part in b_parts(l, g):
                    b_copy(l, g, part, d).wait_send()
        for side in range(2):
            halo_copy(l, side).wait_send()
    for g in range(GROUPS):
        store(g).wait()


def body(ocean_state, zonal_kernel, norm_gain, input_weight, output_weight):
    total = ROWS * lax.axis_size("lat")
    quad = jnp.asarray(row_weights(total))
    table = jnp.asarray(basis().astype(jnp.bfloat16))
    state = jnp.transpose(ocean_state, (0, 1, 3, 2))
    hbm = pl.BlockSpec(memory_space=pl.ANY)
    out = pl.pallas_call(
        kernel,
        out_shape=jax.ShapeDtypeStruct((1, ROWS, COLS, C), BF16),
        in_specs=[
            pl.BlockSpec(memory_space=pltpu.SMEM),
            pl.BlockSpec(memory_space=pltpu.VMEM),
            hbm, hbm, hbm, hbm, hbm,
        ],
        out_specs=hbm,
        scratch_shapes=[
            pltpu.VMEM((ROWS, COLS, C), BF16),
            pltpu.VMEM((2, TILES, C, 128), BF16),
            pltpu.VMEM((2, LON, TILES, SHARE, 128), BF16),
            pltpu.VMEM((2, ROWS + 4, SHARE, W), BF16),
            pltpu.VMEM((ROWS + 4, SHARE, W), F32),
            pltpu.VMEM((2, KROWS, 3, SHARE, HALF), F32),
            pltpu.VMEM((4, SHARE, W), BF16),
            pltpu.VMEM((2, LON, TILES, SHARE, 128), BF16),
            pltpu.VMEM((2, TILES, C, 128), BF16),
            pltpu.VMEM((2, FF, C), BF16),
            pltpu.VMEM((2, C, FF), BF16),
            pltpu.VMEM((FF, 384), BF16),
            pltpu.VMEM((C, 384), BF16),
            pltpu.VMEM((2, C, 128), F32),
            pltpu.VMEM((W, W), BF16),
            pltpu.VMEM((W, W), BF16),
            pltpu.VMEM((BLOCKS, KROWS, TAPS, C), BF16),
            pltpu.VMEM((BLOCKS, C, FF), BF16),
            pltpu.VMEM((BLOCKS, FF, C), BF16),
            pltpu.SemaphoreType.DMA((GROUPS,)),
            pltpu.SemaphoreType.DMA((4,)),
            pltpu.SemaphoreType.DMA((GROUPS,)),
            pltpu.SemaphoreType.DMA((2, GROUPS + 1, LON - 1)),
            pltpu.SemaphoreType.DMA((2, GROUPS + 1, LON - 1)),
            pltpu.SemaphoreType.DMA((2, GROUPS + 1, LON - 1)),
            pltpu.SemaphoreType.DMA((2, GROUPS + 1, LON - 1)),
            pltpu.SemaphoreType.DMA((2, 2)),
            pltpu.SemaphoreType.DMA((2, 2)),
        ],
        compiler_params=pltpu.CompilerParams(
            collective_id=0, has_side_effects=True, vmem_limit_bytes=62 * 1024 * 1024
        ),
    )(quad, norm_gain, state, zonal_kernel, input_weight, output_weight, table)
    return jnp.transpose(out, (0, 1, 3, 2))


def solution(mesh):
    in_specs = (P(None, "lat", None, "lon"), P(), P(), P(), P())
    out_specs = P(None, "lat", None, "lon")
    return jax.shard_map(body, mesh=mesh, in_specs=in_specs, out_specs=out_specs, check_vma=False)
```

```python
import functools

import numpy as np
import jax
import jax.numpy as jnp
from jax import lax
from jax.experimental import pallas as pl
from jax.experimental.pallas import tpu as pltpu
from jax.sharding import PartitionSpec as P

C = 640
FF = 1280
W = 768
TAPS = 256
KROWS = 5
BLOCKS = 2
LON = 8
ROWS = 12
COLS = W // LON
HALF = W // 2
GROUPS = 3
SPLIT = 32
SHARE = C // LON
A_PARTS = (((0, 0, SHARE),), ((1, 0, SHARE),), ((2, 0, SPLIT), (3, SPLIT, SHARE - SPLIT)))
B_PARTS = (((0, 0, SPLIT), (1, SPLIT, SHARE - SPLIT)), ((2, 0, SHARE),), ((3, 0, SHARE),))
TILES = 9
MESH = pl.DeviceIdType.MESH
F32 = jnp.float32
BF16 = jnp.bfloat16


def unit_place(unit):
    device, third = divmod(unit, 3)
    half, quarter = divmod(device, 4)
    return ((2 * third + half) * 4 + quarter) * 32


def basis():
    w = np.arange(W)[:, None]
    f = np.arange(HALF)[None, :]
    angle = 2.0 * np.pi / W * ((w * f) % W)
    sine = np.where(f == 0, 1.0 - 2.0 * (w % 2), np.sin(angle))
    full = np.concatenate([np.cos(angle), sine], axis=1)
    placed = np.zeros_like(full)
    for unit in range(W // 32):
        at = unit_place(unit)
        placed[at : at + 32] = full[32 * unit : 32 * unit + 32]
    return placed


def row_weights(total):
    h = np.arange(total)
    quad = np.sin(np.pi * (h + 0.5) / total)
    return np.concatenate([np.zeros(2), quad, np.zeros(2)]).astype(np.float32)


def nt(a, b):
    return lax.dot_general(a, b, (((1,), (1,)), ((), ())), preferred_element_type=F32)


def nn(a, b):
    return lax.dot_general(a, b, (((1,), (0,)), ((), ())), preferred_element_type=F32)


def gelu(x):
    return 0.5 * x * (1.0 + lax.erf(x * 0.7071067811865476))


def swap4(tiles):
    v0, v1, v2, v3 = tiles
    lane = lax.broadcasted_iota(jnp.int32, v0.shape, 1)
    low = lane < 64
    even = (lane & 32) == 0
    roll = lambda v, s: pltpu.roll(v, s, 1)
    u0 = jnp.where(low, v0, roll(v2, 64))
    u2 = jnp.where(low, roll(v0, 64), v2)
    u1 = jnp.where(low, v1, roll(v3, 64))
    u3 = jnp.where(low, roll(v1, 64), v3)
    return (
        jnp.where(even, u0, roll(u1, 32)),
        jnp.where(even, roll(u0, 96), u1),
        jnp.where(even, u2, roll(u3, 32)),
        jnp.where(even, roll(u2, 96), u3),
    )


def loop(count, body):
    def step(i, carry):
        body(i)
        return carry

    lax.fori_loop(0, count, step, 0)


def kernel(
    quad_ref, gain_ref, x_hbm, kern_hbm, w1_hbm, w2_hbm, f_hbm, out_ref,
    rows_in, xpos, r1, xr, spec, kf, yb, s2, r2, w1t, w2t, hid, nrm, gainb,
    fb, fbt, kraw, w1, w2,
    in_sem, load_sem, a_send, a_recv, b_send, b_recv, h_send, h_recv,
):
    me = lax.axis_index("lon")
    lat = lax.axis_index("lat")
    lats = lax.axis_size("lat")
    up = lax.rem(lat + lats - 1, lats)
    down = lax.rem(lat + 1, lats)
    mine = pl.ds(pl.multiple_of(me * SHARE, SHARE), SHARE)

    def tiles_of(g):
        return pl.ds(3 * g, 3)

    def fetch(g):
        return pltpu.make_async_copy(
            x_hbm.at[0, pl.ds(4 * g, 4)], rows_in.at[pl.ds(4 * g, 4)], in_sem.at[g]
        )

    for g in (1, 0, 2):
        fetch(g).start()
    loads = [
        pltpu.make_async_copy(src, dst, load_sem.at[i])
        for i, (src, dst) in enumerate(
            [(kern_hbm, kraw), (f_hbm, fb), (w1_hbm, w1), (w2_hbm, w2)]
        )
    ]
    for copy in loads:
        copy.start()

    barrier = pltpu.get_barrier_semaphore()
    for d in range(1, LON):
        pl.semaphore_signal(
            barrier, inc=1, device_id={"lon": lax.rem(me + d, LON)}, device_id_type=MESH
        )
    for other in (up, down):
        pl.semaphore_signal(barrier, inc=1, device_id={"lat": other}, device_id_type=MESH)

    def channels(owner, first, count):
        return pl.ds(pl.multiple_of(owner * SHARE + first, 16), count)

    def a_copy(l, g, part, d):
        slot, first, count = part
        peer = lax.rem(me + d, LON)
        return pltpu.make_async_remote_copy(
            src_ref=xpos.at[l, tiles_of(g), channels(peer, first, count)],
            dst_ref=r1.at[l, me, tiles_of(g), pl.ds(first, count)],
            send_sem=a_send.at[l, slot, d - 1],
            recv_sem=a_recv.at[l, slot, d - 1],
            device_id={"lon": peer},
            device_id_type=MESH,
        )

    def b_copy(l, g, part, d):
        slot, first, count = part
        peer = lax.rem(me + d, LON)
        return pltpu.make_async_remote_copy(
            src_ref=s2.at[l, peer, tiles_of(g), pl.ds(first, count)],
            dst_ref=r2.at[l, tiles_of(g), channels(me, first, count)],
            send_sem=b_send.at[l, slot, d - 1],
            recv_sem=b_recv.at[l, slot, d - 1],
            device_id={"lon": peer},
            device_id_type=MESH,
        )

    def halo_copy(l, g):
        return pltpu.make_async_remote_copy(
            src_ref=xr.at[l, pl.ds(2 + 5 * g, 2)],
            dst_ref=xr.at[l, pl.ds(14 - 7 * g, 2)],
            send_sem=h_send.at[l, g // 2],
            recv_sem=h_recv.at[l, g // 2],
            device_id={"lat": lax.rem(lat + lats + g - 1, lats)},
            device_id_type=MESH,
        )

    def start_a(l, g, place):
        for part in A_PARTS[place]:
            for d in range(1, LON):
                a_copy(l, g, part, d).start()
        r1[l, me, tiles_of(g)] = xpos[l, tiles_of(g), mine]

    def pack_input(g):
        def piece(i):
            at = pl.ds(pl.multiple_of(i * 128, 128), 128)
            for third in range(3):
                lons = pl.ds(32 * third, 32)
                tile = jnp.concatenate([rows_in[4 * g + r, lons, at] for r in range(4)], axis=0)
                xpos[0, 3 * g + third, at, :] = tile.T

        loop(C // 128, piece)

    for place, g in enumerate((1, 0, 2)):
        fetch(g).wait()
        pack_input(g)
        if place == 0:
            pl.semaphore_wait(barrier, LON + 1)
        start_a(0, g, place)

    def unit_matrix(n):
        return (
            lax.broadcasted_iota(jnp.int32, (n, n), 0)
            == lax.broadcasted_iota(jnp.int32, (n, n), 1)
        ).astype(BF16)

    loads[0].wait()
    loads[1].wait()
    taps_basis = [unit_place((32 * u - TAPS // 2) % W // 32) for u in range(TAPS // 32)]

    def spectra(i):
        l = i // KROWS
        r = lax.rem(i, KROWS)
        pick = (
            lax.broadcasted_iota(jnp.int32, (SHARE, C), 1)
            == lax.broadcasted_iota(jnp.int32, (SHARE, C), 0) + me * SHARE
        ).astype(BF16)
        taps = nt(pick, kraw[l, r]).astype(BF16)
        tap_rows = jnp.concatenate([fb[p : p + 32, :] for p in taps_basis], axis=0)
        full = nn(taps, tap_rows)
        keep = lax.broadcasted_iota(jnp.int32, (SHARE, HALF), 1) >= 1
        scale = jnp.where(keep, 2.0 / W, 1.0 / W).astype(F32)
        real = full[:, :HALF] * scale
        sine = full[:, HALF:] * scale
        kf[l, r, 0] = real
        kf[l, r, 1] = jnp.where(keep, sine, 0.0)
        kf[l, r, 2] = jnp.where(keep, real, sine)

    loop(BLOCKS * KROWS, spectra)

    def turn0(i):
        at = pl.ds(pl.multiple_of(i * 256, 256), 256)
        fbt[at, :] = nt(unit_matrix(256), fb[:, at]).astype(BF16)

    loop(W // 256, turn0)
    loads[2].wait()
    loads[3].wait()

    for l in range(BLOCKS):

        def turn1(i):
            at = pl.ds(pl.multiple_of(i * 256, 256), 256)
            w1t[l, at, :] = nt(unit_matrix(256), w1[l, :, at]).astype(BF16)

        def turn2(i):
            at = pl.ds(pl.multiple_of(i * 128, 128), 128)
            w2t[l, at, :] = nt(unit_matrix(128), w2[l, :, at]).astype(BF16)
            row = jnp.broadcast_to(gain_ref[pl.ds(l, 1), at].astype(F32), (128, 128))
            gainb[l, at, :] = row.T

        loop(FF // 256, turn1)
        loop(C // 128, turn2)

    def unpack(l, g, first, count):
        some = pl.ds(first, count)

        def piece(third):
            for half in range(2):
                tiles = [r1[l, 4 * half + q, 3 * g + third, some, :] for q in range(4)]
                rows = swap4(tiles)
                at = pl.ds(pl.multiple_of(256 * third, 128) + 128 * half, 128)
                for r in range(4):
                    xr[l, 2 + 4 * g + r, some, at] = rows[r]

        loop(3, piece)

    def transform(l, top, rows, first, count):
        some = pl.ds(first, count)
        lhs = xr[l, pl.ds(top, rows), some, :].reshape(rows * count, W)
        for n in range(3):
            at = pl.ds(256 * n, 256)
            part = nn(lhs, fb[:, at])
            for r in range(rows):
                weight = quad_ref[lat * ROWS + top + r]
                spec[top + r, some, at] = part[count * r : count * (r + 1)] * weight

    def convolve(l, g, first, count):
        some = pl.ds(first, count)

        def bands(i):
            rows = pl.ds(pl.multiple_of(first + i * 16, 16), 16)
            for n in range(3):
                re_at = pl.ds(128 * n, 128)
                im_at = pl.ds(HALF + 128 * n, 128)
                factors = [
                    [kf[l, r, j, rows, re_at] for j in range(3)] for r in range(KROWS)
                ]
                for row in range(4):
                    real = sine = None
                    for r in range(KROWS):
                        a = spec[4 * g + row + r, rows, re_at]
                        b = spec[4 * g + row + r, rows, im_at]
                        kr, kc, ks = factors[r]
                        new_real = a * kr - b * kc
                        new_sine = a * kc + b * ks
                        real = new_real if real is None else real + new_real
                        sine = new_sine if sine is None else sine + new_sine
                    yb[row, rows, re_at] = real.astype(BF16)
                    yb[row, rows, im_at] = sine.astype(BF16)

        loop(count // 16, bands)

        lhs = yb[:, some, :].reshape(4 * count, W)
        for third in range(3):
            at = 256 * third
            part = nn(lhs, fbt[:, pl.ds(at, 256)])
            for half in range(2):
                tiles = []
                for r in range(4):
                    conv = part[count * r : count * (r + 1), 128 * half : 128 * (half + 1)]
                    old = xr[l, 2 + 4 * g + r, some, pl.ds(at + 128 * half, 128)]
                    tiles.append((old.astype(F32) + gelu(conv)).astype(BF16))
                packed = swap4(tiles)
                for q in range(4):
                    s2[l, 4 * half + q, 3 * g + third, some, :] = packed[q]

    def start_b(l, g, part):
        slot, first, count = part
        for d in range(1, LON):
            b_copy(l, g, part, d).start()
        r2[l, tiles_of(g), channels(me, first, count)] = s2[
            l, me, tiles_of(g), pl.ds(first, count)
        ]

    def feed_forward(l, g):
        def norm(t):
            values = r2[l, 3 * g + t].astype(F32)
            average = jnp.sum(values, axis=0, keepdims=True) * (1.0 / C)
            centred = values - average
            variance = jnp.sum(centred * centred, axis=0, keepdims=True) * (1.0 / C)
            scaled = centred * lax.rsqrt(variance + 1e-05) * gainb[l]
            nrm[:, pl.ds(pl.multiple_of(128 * t, 128), 128)] = scaled.astype(BF16)

        loop(3, norm)

        for i in range(FF // 256):
            at = pl.ds(i * 256, 256)
            hid[at, :] = gelu(nn(w1t[l, at, :], nrm[...])).astype(BF16)
        out = nn(w2t[l], hid[...])
        for t in range(3):
            old = r2[l, 3 * g + t].astype(F32)
            new = (old + out[:, 128 * t : 128 * (t + 1)]).astype(BF16)
            xpos[1 - l, 3 * g + t] = new

    def finish(g):
        def piece(i):
            at = pl.ds(pl.multiple_of(i * 128, 128), 128)
            for third in range(3):
                turned = xpos[0, 3 * g + third, at, :].T
                for r in range(4):
                    out_ref[0, 4 * g + r, pl.ds(32 * third, 32), at] = turned[
                        32 * r : 32 * (r + 1), :
                    ]

        loop(C // 128, piece)

    def take(l, g, part):
        for d in range(1, LON):
            a_copy(l, g, part, d).wait_recv()
        unpack(l, g, *part[1:])
        transform(l, 2 + 4 * g, 4, *part[1:])

    def give(l, g, part):
        convolve(l, g, *part[1:])
        start_b(l, g, part)

    def block(l):
        early, late = 2 * l, 2 - 2 * l
        take(l, 1, A_PARTS[0][0])
        take(l, early, A_PARTS[1][0])
        halo_copy(l, early).start()
        for place, (arrived, ready) in enumerate(zip(A_PARTS[2], B_PARTS[0])):
            take(l, late, arrived)
            if place == 1:
                halo_copy(l, late).start()
            give(l, 1, ready)
        for place, g in ((1, late), (2, early)):
            halo_copy(l, 2 - g).wait_recv()
            transform(l, 7 * g, 2, 0, SHARE)
            give(l, g, B_PARTS[place][0])
        for place, g in enumerate((1, late, early)):
            for part in B_PARTS[place]:
                for d in range(1, LON):
                    b_copy(l, g, part, d).wait_recv()
            feed_forward(l, g)

            @pl.when(l == 0)
            def _():
                start_a(1, g, place)

            @pl.when(l == BLOCKS - 1)
            def _():
                finish(g)

        for a_place, g in enumerate((1, early, late)):
            for d in range(1, LON):
                for part in A_PARTS[a_place]:
                    a_copy(l, g, part, d).wait_send()
        for b_place, g in enumerate((1, late, early)):
            for d in range(1, LON):
                for part in B_PARTS[b_place]:
                    b_copy(l, g, part, d).wait_send()
        halo_copy(l, early).wait_send()
        halo_copy(l, late).wait_send()

    loop(BLOCKS, block)


def body(ocean_state, zonal_kernel, norm_gain, input_weight, output_weight):
    total = ROWS * lax.axis_size("lat")
    quad = jnp.asarray(row_weights(total))
    table = jnp.asarray(basis().astype(jnp.bfloat16))
    state = jnp.transpose(ocean_state, (0, 1, 3, 2))
    hbm = pl.BlockSpec(memory_space=pl.ANY)
    out = pl.pallas_call(
        kernel,
        out_shape=pltpu.VMEM((1, ROWS, COLS, C), BF16),
        in_specs=[
            pl.BlockSpec(memory_space=pltpu.SMEM),
            pl.BlockSpec(memory_space=pltpu.VMEM),
            hbm, hbm, hbm, hbm, hbm,
        ],
        out_specs=pl.BlockSpec(memory_space=pltpu.VMEM),
        scratch_shapes=[
            pltpu.VMEM((ROWS, COLS, C), BF16),
            pltpu.VMEM((2, TILES, C, 128), BF16),
            pltpu.VMEM((2, LON, TILES, SHARE, 128), BF16),
            pltpu.VMEM((2, ROWS + 4, SHARE, W), BF16),
            pltpu.VMEM((ROWS + 4, SHARE, W), F32),
            pltpu.VMEM((2, KROWS, 3, SHARE, HALF), F32),
            pltpu.VMEM((4, SHARE, W), BF16),
            pltpu.VMEM((2, LON, TILES, SHARE, 128), BF16),
            pltpu.VMEM((2, TILES, C, 128), BF16),
            pltpu.VMEM((2, FF, C), BF16),
            pltpu.VMEM((2, C, FF), BF16),
            pltpu.VMEM((FF, 384), BF16),
            pltpu.VMEM((C, 384), BF16),
            pltpu.VMEM((2, C, 128), F32),
            pltpu.VMEM((W, W), BF16),
            pltpu.VMEM((W, W), BF16),
            pltpu.VMEM((BLOCKS, KROWS, TAPS, C), BF16),
            pltpu.VMEM((BLOCKS, C, FF), BF16),
            pltpu.VMEM((BLOCKS, FF, C), BF16),
            pltpu.SemaphoreType.DMA((GROUPS,)),
            pltpu.SemaphoreType.DMA((4,)),
            pltpu.SemaphoreType.DMA((2, GROUPS + 1, LON - 1)),
            pltpu.SemaphoreType.DMA((2, GROUPS + 1, LON - 1)),
            pltpu.SemaphoreType.DMA((2, GROUPS + 1, LON - 1)),
            pltpu.SemaphoreType.DMA((2, GROUPS + 1, LON - 1)),
            pltpu.SemaphoreType.DMA((2, 2)),
            pltpu.SemaphoreType.DMA((2, 2)),
        ],
        compiler_params=pltpu.CompilerParams(
            collective_id=0, has_side_effects=True, vmem_limit_bytes=54 * 1024 * 1024
        ),
    )(quad, norm_gain, state, zonal_kernel, input_weight, output_weight, table)
    return jnp.transpose(out, (0, 1, 3, 2))


def solution(mesh):
    in_specs = (P(None, "lat", None, "lon"), P(), P(), P(), P())
    out_specs = P(None, "lat", None, "lon")
    return jax.shard_map(body, mesh=mesh, in_specs=in_specs, out_specs=out_specs, check_vma=False)
```

```python
import functools

import numpy as np
import jax
import jax.numpy as jnp
from jax import lax
from jax.experimental import pallas as pl
from jax.experimental.pallas import tpu as pltpu
from jax.sharding import PartitionSpec as P

C = 640
FF = 1280
W = 768
TAPS = 256
KROWS = 5
BLOCKS = 2
LON = 8
ROWS = 12
COLS = W // LON
HALF = W // 2
GROUPS = 3
SPLIT = 48
SHARE = C // LON
A_PARTS = (((0, 0, SHARE),), ((1, 0, SHARE),), ((2, 0, SPLIT), (3, SPLIT, SHARE - SPLIT)))
B_PARTS = (((0, 0, SPLIT), (1, SPLIT, SHARE - SPLIT)), ((2, 0, SHARE),), ((3, 0, SHARE),))
TILES = 9
MESH = pl.DeviceIdType.MESH
F32 = jnp.float32
BF16 = jnp.bfloat16


def unit_place(unit):
    device, third = divmod(unit, 3)
    half, quarter = divmod(device, 4)
    return ((2 * third + half) * 4 + quarter) * 32


def basis():
    w = np.arange(W)[:, None]
    f = np.arange(HALF)[None, :]
    angle = 2.0 * np.pi / W * ((w * f) % W)
    sine = np.where(f == 0, 1.0 - 2.0 * (w % 2), np.sin(angle))
    full = np.concatenate([np.cos(angle), sine], axis=1)
    placed = np.zeros_like(full)
    for unit in range(W // 32):
        at = unit_place(unit)
        placed[at : at + 32] = full[32 * unit : 32 * unit + 32]
    return placed


def row_weights(total):
    h = np.arange(total)
    quad = np.sin(np.pi * (h + 0.5) / total)
    return np.concatenate([np.zeros(2), quad, np.zeros(2)]).astype(np.float32)


def nt(a, b):
    return lax.dot_general(a, b, (((1,), (1,)), ((), ())), preferred_element_type=F32)


def nn(a, b):
    return lax.dot_general(a, b, (((1,), (0,)), ((), ())), preferred_element_type=F32)


def gelu(x):
    return 0.5 * x * (1.0 + lax.erf(x * 0.7071067811865476))


def swap4(tiles):
    v0, v1, v2, v3 = tiles
    lane = lax.broadcasted_iota(jnp.int32, v0.shape, 1)
    low = lane < 64
    even = (lane & 32) == 0
    roll = lambda v, s: pltpu.roll(v, s, 1)
    u0 = jnp.where(low, v0, roll(v2, 64))
    u2 = jnp.where(low, roll(v0, 64), v2)
    u1 = jnp.where(low, v1, roll(v3, 64))
    u3 = jnp.where(low, roll(v1, 64), v3)
    return (
        jnp.where(even, u0, roll(u1, 32)),
        jnp.where(even, roll(u0, 96), u1),
        jnp.where(even, u2, roll(u3, 32)),
        jnp.where(even, roll(u2, 96), u3),
    )


def loop(count, body):
    def step(i, carry):
        body(i)
        return carry

    lax.fori_loop(0, count, step, 0)


def kernel(
    quad_ref, gain_ref, x_hbm, kern_hbm, w1_hbm, w2_hbm, f_hbm, out_ref,
    rows_in, xpos, r1, xr, spec, kf, yb, s2, r2, w1t, w2t, hid, nrm, gainb,
    fb, fbt, kraw, w1, w2,
    in_sem, load_sem, a_send, a_recv, b_send, b_recv, h_send, h_recv,
):
    me = lax.axis_index("lon")
    lat = lax.axis_index("lat")
    lats = lax.axis_size("lat")
    up = lax.rem(lat + lats - 1, lats)
    down = lax.rem(lat + 1, lats)
    mine = pl.ds(pl.multiple_of(me * SHARE, SHARE), SHARE)

    def tiles_of(g):
        return pl.ds(3 * g, 3)

    def fetch(g):
        return pltpu.make_async_copy(
            x_hbm.at[0, pl.ds(4 * g, 4)], rows_in.at[pl.ds(4 * g, 4)], in_sem.at[g]
        )

    for g in (1, 0, 2):
        fetch(g).start()
    loads = [
        pltpu.make_async_copy(src, dst, load_sem.at[i])
        for i, (src, dst) in enumerate(
            [(kern_hbm, kraw), (f_hbm, fb), (w1_hbm, w1), (w2_hbm, w2)]
        )
    ]
    for copy in loads:
        copy.start()

    barrier = pltpu.get_barrier_semaphore()
    for d in range(1, LON):
        pl.semaphore_signal(
            barrier, inc=1, device_id={"lon": lax.rem(me + d, LON)}, device_id_type=MESH
        )
    for other in (up, down):
        pl.semaphore_signal(barrier, inc=1, device_id={"lat": other}, device_id_type=MESH)

    def channels(owner, first, count):
        return pl.ds(pl.multiple_of(owner * SHARE + first, 16), count)

    def a_copy(l, g, part, d):
        slot, first, count = part
        peer = lax.rem(me + d, LON)
        return pltpu.make_async_remote_copy(
            src_ref=xpos.at[l, tiles_of(g), channels(peer, first, count)],
            dst_ref=r1.at[l, me, tiles_of(g), pl.ds(first, count)],
            send_sem=a_send.at[l, slot, d - 1],
            recv_sem=a_recv.at[l, slot, d - 1],
            device_id={"lon": peer},
            device_id_type=MESH,
        )

    def b_copy(l, g, part, d):
        slot, first, count = part
        peer = lax.rem(me + d, LON)
        return pltpu.make_async_remote_copy(
            src_ref=s2.at[l, peer, tiles_of(g), pl.ds(first, count)],
            dst_ref=r2.at[l, tiles_of(g), channels(me, first, count)],
            send_sem=b_send.at[l, slot, d - 1],
            recv_sem=b_recv.at[l, slot, d - 1],
            device_id={"lon": peer},
            device_id_type=MESH,
        )

    def halo_copy(l, g):
        return pltpu.make_async_remote_copy(
            src_ref=xr.at[l, pl.ds(2 + 5 * g, 2)],
            dst_ref=xr.at[l, pl.ds(14 - 7 * g, 2)],
            send_sem=h_send.at[l, g // 2],
            recv_sem=h_recv.at[l, g // 2],
            device_id={"lat": lax.rem(lat + lats + g - 1, lats)},
            device_id_type=MESH,
        )

    def start_a(l, g, place):
        for part in A_PARTS[place]:
            for d in range(1, LON):
                a_copy(l, g, part, d).start()
        r1[l, me, tiles_of(g)] = xpos[l, tiles_of(g), mine]

    def pack_input(g):
        def piece(i):
            at = pl.ds(pl.multiple_of(i * 128, 128), 128)
            for third in range(3):
                lons = pl.ds(32 * third, 32)
                tile = jnp.concatenate([rows_in[4 * g + r, lons, at] for r in range(4)], axis=0)
                xpos[0, 3 * g + third, at, :] = tile.T

        loop(C // 128, piece)

    for place, g in enumerate((1, 0, 2)):
        fetch(g).wait()
        pack_input(g)
        if place == 0:
            pl.semaphore_wait(barrier, LON + 1)
        start_a(0, g, place)

    def unit_matrix(n):
        return (
            lax.broadcasted_iota(jnp.int32, (n, n), 0)
            == lax.broadcasted_iota(jnp.int32, (n, n), 1)
        ).astype(BF16)

    loads[0].wait()
    loads[1].wait()
    taps_basis = [unit_place((32 * u - TAPS // 2) % W // 32) for u in range(TAPS // 32)]

    def spectra(i):
        l = i // KROWS
        r = lax.rem(i, KROWS)
        pick = (
            lax.broadcasted_iota(jnp.int32, (SHARE, C), 1)
            == lax.broadcasted_iota(jnp.int32, (SHARE, C), 0) + me * SHARE
        ).astype(BF16)
        taps = nt(pick, kraw[l, r]).astype(BF16)
        tap_rows = jnp.concatenate([fb[p : p + 32, :] for p in taps_basis], axis=0)
        full = nn(taps, tap_rows)
        keep = lax.broadcasted_iota(jnp.int32, (SHARE, HALF), 1) >= 1
        scale = jnp.where(keep, 2.0 / W, 1.0 / W).astype(F32)
        real = full[:, :HALF] * scale
        sine = full[:, HALF:] * scale
        kf[l, r, 0] = real
        kf[l, r, 1] = jnp.where(keep, sine, 0.0)
        kf[l, r, 2] = jnp.where(keep, real, sine)

    loop(BLOCKS * KROWS, spectra)

    def turn0(i):
        at = pl.ds(pl.multiple_of(i * 256, 256), 256)
        fbt[at, :] = nt(unit_matrix(256), fb[:, at]).astype(BF16)

    loop(W // 256, turn0)
    loads[2].wait()
    loads[3].wait()

    for l in range(BLOCKS):

        def turn1(i):
            at = pl.ds(pl.multiple_of(i * 256, 256), 256)
            w1t[l, at, :] = nt(unit_matrix(256), w1[l, :, at]).astype(BF16)

        def turn2(i):
            at = pl.ds(pl.multiple_of(i * 128, 128), 128)
            w2t[l, at, :] = nt(unit_matrix(128), w2[l, :, at]).astype(BF16)
            row = jnp.broadcast_to(gain_ref[pl.ds(l, 1), at].astype(F32), (128, 128))
            gainb[l, at, :] = row.T

        loop(FF // 256, turn1)
        loop(C // 128, turn2)

    def unpack(l, g, first, count):
        some = pl.ds(first, count)

        def piece(third):
            for half in range(2):
                tiles = [r1[l, 4 * half + q, 3 * g + third, some, :] for q in range(4)]
                rows = swap4(tiles)
                at = pl.ds(pl.multiple_of(256 * third, 128) + 128 * half, 128)
                for r in range(4):
                    xr[l, 2 + 4 * g + r, some, at] = rows[r]

        loop(3, piece)

    def transform(l, top, rows, first, count):
        some = pl.ds(first, count)
        lhs = xr[l, pl.ds(top, rows), some, :].reshape(rows * count, W)
        for n in range(3):
            at = pl.ds(256 * n, 256)
            part = nn(lhs, fb[:, at])
            for r in range(rows):
                weight = quad_ref[lat * ROWS + top + r]
                spec[top + r, some, at] = part[count * r : count * (r + 1)] * weight

    def convolve(l, g, first, count):
        some = pl.ds(first, count)

        def bands(i):
            rows = pl.ds(pl.multiple_of(first + i * 16, 16), 16)
            for n in range(3):
                re_at = pl.ds(128 * n, 128)
                im_at = pl.ds(HALF + 128 * n, 128)
                factors = [
                    [kf[l, r, j, rows, re_at] for j in range(3)] for r in range(KROWS)
                ]
                for row in range(4):
                    real = sine = None
                    for r in range(KROWS):
                        a = spec[4 * g + row + r, rows, re_at]
                        b = spec[4 * g + row + r, rows, im_at]
                        kr, kc, ks = factors[r]
                        new_real = a * kr - b * kc
                        new_sine = a * kc + b * ks
                        real = new_real if real is None else real + new_real
                        sine = new_sine if sine is None else sine + new_sine
                    yb[row, rows, re_at] = real.astype(BF16)
                    yb[row, rows, im_at] = sine.astype(BF16)

        loop(count // 16, bands)

        lhs = yb[:, some, :].reshape(4 * count, W)
        for third in range(3):
            at = 256 * third
            part = nn(lhs, fbt[:, pl.ds(at, 256)])
            for half in range(2):
                tiles = []
                for r in range(4):
                    conv = part[count * r : count * (r + 1), 128 * half : 128 * (half + 1)]
                    old = xr[l, 2 + 4 * g + r, some, pl.ds(at + 128 * half, 128)]
                    tiles.append((old.astype(F32) + gelu(conv)).astype(BF16))
                packed = swap4(tiles)
                for q in range(4):
                    s2[l, 4 * half + q, 3 * g + third, some, :] = packed[q]

    def start_b(l, g, part):
        slot, first, count = part
        for d in range(1, LON):
            b_copy(l, g, part, d).start()
        r2[l, tiles_of(g), channels(me, first, count)] = s2[
            l, me, tiles_of(g), pl.ds(first, count)
        ]

    def feed_forward(l, g):
        def norm(t):
            values = r2[l, 3 * g + t].astype(F32)
            average = jnp.sum(values, axis=0, keepdims=True) * (1.0 / C)
            centred = values - average
            variance = jnp.sum(centred * centred, axis=0, keepdims=True) * (1.0 / C)
            scaled = centred * lax.rsqrt(variance + 1e-05) * gainb[l]
            nrm[:, pl.ds(pl.multiple_of(128 * t, 128), 128)] = scaled.astype(BF16)

        loop(3, norm)

        for i in range(FF // 256):
            at = pl.ds(i * 256, 256)
            hid[at, :] = gelu(nn(w1t[l, at, :], nrm[...])).astype(BF16)
        out = nn(w2t[l], hid[...])
        for t in range(3):
            old = r2[l, 3 * g + t].astype(F32)
            new = (old + out[:, 128 * t : 128 * (t + 1)]).astype(BF16)
            xpos[1 - l, 3 * g + t] = new

    def finish(g):
        def piece(i):
            at = pl.ds(pl.multiple_of(i * 128, 128), 128)
            for third in range(3):
                turned = xpos[0, 3 * g + third, at, :].T
                for r in range(4):
                    out_ref[0, 4 * g + r, pl.ds(32 * third, 32), at] = turned[
                        32 * r : 32 * (r + 1), :
                    ]

        loop(C // 128, piece)

    def take(l, g, part, rim=False):
        for d in range(1, LON):
            a_copy(l, g, part, d).wait_recv()
        unpack(l, g, *part[1:])
        if rim:
            halo_copy(l, g).start()
        transform(l, 2 + 4 * g, 4, *part[1:])

    def take_rim(l, g):
        halo_copy(l, 2 - g).wait_recv()
        transform(l, 7 * g, 2, 0, SHARE)

    def give(l, g, part):
        convolve(l, g, *part[1:])
        start_b(l, g, part)

    def block(l):
        early, late = 2 * l, 2 - 2 * l
        take(l, 1, A_PARTS[0][0])
        take(l, early, A_PARTS[1][0], rim=True)
        take(l, late, A_PARTS[2][0])
        give(l, 1, B_PARTS[0][0])
        take_rim(l, late)
        take(l, late, A_PARTS[2][1], rim=True)
        give(l, 1, B_PARTS[0][1])
        give(l, late, B_PARTS[1][0])
        take_rim(l, early)
        give(l, early, B_PARTS[2][0])
        for place, g in enumerate((1, late, early)):
            for part in B_PARTS[place]:
                for d in range(1, LON):
                    b_copy(l, g, part, d).wait_recv()
            feed_forward(l, g)

            @pl.when(l == 0)
            def _():
                start_a(1, g, place)

            @pl.when(l == BLOCKS - 1)
            def _():
                finish(g)

        for a_place, g in enumerate((1, early, late)):
            for d in range(1, LON):
                for part in A_PARTS[a_place]:
                    a_copy(l, g, part, d).wait_send()
        for b_place, g in enumerate((1, late, early)):
            for d in range(1, LON):
                for part in B_PARTS[b_place]:
                    b_copy(l, g, part, d).wait_send()
        halo_copy(l, early).wait_send()
        halo_copy(l, late).wait_send()

    loop(BLOCKS, block)


def body(ocean_state, zonal_kernel, norm_gain, input_weight, output_weight):
    total = ROWS * lax.axis_size("lat")
    quad = jnp.asarray(row_weights(total))
    table = jnp.asarray(basis().astype(jnp.bfloat16))
    state = jnp.transpose(ocean_state, (0, 1, 3, 2))
    hbm = pl.BlockSpec(memory_space=pl.ANY)
    out = pl.pallas_call(
        kernel,
        out_shape=pltpu.VMEM((1, ROWS, COLS, C), BF16),
        in_specs=[
            pl.BlockSpec(memory_space=pltpu.SMEM),
            pl.BlockSpec(memory_space=pltpu.VMEM),
            hbm, hbm, hbm, hbm, hbm,
        ],
        out_specs=pl.BlockSpec(memory_space=pltpu.VMEM),
        scratch_shapes=[
            pltpu.VMEM((ROWS, COLS, C), BF16),
            pltpu.VMEM((2, TILES, C, 128), BF16),
            pltpu.VMEM((2, LON, TILES, SHARE, 128), BF16),
            pltpu.VMEM((2, ROWS + 4, SHARE, W), BF16),
            pltpu.VMEM((ROWS + 4, SHARE, W), F32),
            pltpu.VMEM((2, KROWS, 3, SHARE, HALF), F32),
            pltpu.VMEM((4, SHARE, W), BF16),
            pltpu.VMEM((2, LON, TILES, SHARE, 128), BF16),
            pltpu.VMEM((2, TILES, C, 128), BF16),
            pltpu.VMEM((2, FF, C), BF16),
            pltpu.VMEM((2, C, FF), BF16),
            pltpu.VMEM((FF, 384), BF16),
            pltpu.VMEM((C, 384), BF16),
            pltpu.VMEM((2, C, 128), F32),
            pltpu.VMEM((W, W), BF16),
            pltpu.VMEM((W, W), BF16),
            pltpu.VMEM((BLOCKS, KROWS, TAPS, C), BF16),
            pltpu.VMEM((BLOCKS, C, FF), BF16),
            pltpu.VMEM((BLOCKS, FF, C), BF16),
            pltpu.SemaphoreType.DMA((GROUPS,)),
            pltpu.SemaphoreType.DMA((4,)),
            pltpu.SemaphoreType.DMA((2, GROUPS + 1, LON - 1)),
            pltpu.SemaphoreType.DMA((2, GROUPS + 1, LON - 1)),
            pltpu.SemaphoreType.DMA((2, GROUPS + 1, LON - 1)),
            pltpu.SemaphoreType.DMA((2, GROUPS + 1, LON - 1)),
            pltpu.SemaphoreType.DMA((2, 2)),
            pltpu.SemaphoreType.DMA((2, 2)),
        ],
        compiler_params=pltpu.CompilerParams(
            collective_id=0, has_side_effects=True, vmem_limit_bytes=54 * 1024 * 1024
        ),
    )(quad, norm_gain, state, zonal_kernel, input_weight, output_weight, table)
    return jnp.transpose(out, (0, 1, 3, 2))


def solution(mesh):
    in_specs = (P(None, "lat", None, "lon"), P(), P(), P(), P())
    out_specs = P(None, "lat", None, "lon")
    return jax.shard_map(body, mesh=mesh, in_specs=in_specs, out_specs=out_specs, check_vma=False)
```

```python
import functools

import numpy as np
import jax
import jax.numpy as jnp
from jax import lax
from jax.experimental import pallas as pl
from jax.experimental.pallas import tpu as pltpu
from jax.sharding import PartitionSpec as P

C = 640
FF = 1280
W = 768
TAPS = 256
KROWS = 5
BLOCKS = 2
LON = 8
ROWS = 12
COLS = W // LON
HALF = W // 2
GROUPS = 3
SPLIT = 32
SHARE = C // LON
A_PARTS = (((0, 0, SHARE),), ((1, 0, SHARE),), ((2, 0, SPLIT), (3, SPLIT, SHARE - SPLIT)))
B_PARTS = (((0, 0, SPLIT), (1, SPLIT, SHARE - SPLIT)), ((2, 0, SHARE),), ((3, 0, SHARE),))
TILES = 9
MESH = pl.DeviceIdType.MESH
F32 = jnp.float32
BF16 = jnp.bfloat16


def unit_place(unit):
    device, third = divmod(unit, 3)
    half, quarter = divmod(device, 4)
    return ((2 * third + half) * 4 + quarter) * 32


def basis():
    w = np.arange(W)[:, None]
    f = np.arange(HALF)[None, :]
    angle = 2.0 * np.pi / W * ((w * f) % W)
    sine = np.where(f == 0, 1.0 - 2.0 * (w % 2), np.sin(angle))
    full = np.concatenate([np.cos(angle), sine], axis=1)
    placed = np.zeros_like(full)
    for unit in range(W // 32):
        at = unit_place(unit)
        placed[at : at + 32] = full[32 * unit : 32 * unit + 32]
    return placed


def row_weights(total):
    h = np.arange(total)
    quad = np.sin(np.pi * (h + 0.5) / total)
    return np.concatenate([np.zeros(2), quad, np.zeros(2)]).astype(np.float32)


def nt(a, b):
    return lax.dot_general(a, b, (((1,), (1,)), ((), ())), preferred_element_type=F32)


def nn(a, b):
    return lax.dot_general(a, b, (((1,), (0,)), ((), ())), preferred_element_type=F32)


def gelu(x):
    return 0.5 * x * (1.0 + lax.erf(x * 0.7071067811865476))


def swap4(tiles):
    v0, v1, v2, v3 = tiles
    lane = lax.broadcasted_iota(jnp.int32, v0.shape, 1)
    low = lane < 64
    even = (lane & 32) == 0
    roll = lambda v, s: pltpu.roll(v, s, 1)
    u0 = jnp.where(low, v0, roll(v2, 64))
    u2 = jnp.where(low, roll(v0, 64), v2)
    u1 = jnp.where(low, v1, roll(v3, 64))
    u3 = jnp.where(low, roll(v1, 64), v3)
    return (
        jnp.where(even, u0, roll(u1, 32)),
        jnp.where(even, roll(u0, 96), u1),
        jnp.where(even, u2, roll(u3, 32)),
        jnp.where(even, roll(u2, 96), u3),
    )


def loop(count, body):
    def step(i, carry):
        body(i)
        return carry

    lax.fori_loop(0, count, step, 0)


def kernel(
    quad_ref, gain_ref, x_hbm, kern_hbm, w1_hbm, w2_hbm, f_hbm, out_ref,
    rows_in, xpos, r1, xr, spec, kf, yb, s2, r2, w1t, w2t, hid, nrm, gainb,
    fb, fbt, kraw, w1, w2,
    in_sem, load_sem, a_send, a_recv, b_send, b_recv, h_send, h_recv,
):
    me = lax.axis_index("lon")
    lat = lax.axis_index("lat")
    lats = lax.axis_size("lat")
    up = lax.rem(lat + lats - 1, lats)
    down = lax.rem(lat + 1, lats)
    mine = pl.ds(pl.multiple_of(me * SHARE, SHARE), SHARE)

    def tiles_of(g):
        return pl.ds(3 * g, 3)

    def fetch(g):
        return pltpu.make_async_copy(
            x_hbm.at[0, pl.ds(4 * g, 4)], rows_in.at[pl.ds(4 * g, 4)], in_sem.at[g]
        )

    for g in (1, 0, 2):
        fetch(g).start()
    loads = [
        pltpu.make_async_copy(src, dst, load_sem.at[i])
        for i, (src, dst) in enumerate(
            [(kern_hbm, kraw), (f_hbm, fb), (w1_hbm, w1), (w2_hbm, w2)]
        )
    ]
    for copy in loads:
        copy.start()

    barrier = pltpu.get_barrier_semaphore()
    for d in range(1, LON):
        pl.semaphore_signal(
            barrier, inc=1, device_id={"lon": lax.rem(me + d, LON)}, device_id_type=MESH
        )
    for other in (up, down):
        pl.semaphore_signal(barrier, inc=1, device_id={"lat": other}, device_id_type=MESH)

    def channels(owner, first, count):
        return pl.ds(pl.multiple_of(owner * SHARE + first, 16), count)

    def a_copy(l, g, part, d):
        slot, first, count = part
        peer = lax.rem(me + d, LON)
        return pltpu.make_async_remote_copy(
            src_ref=xpos.at[l, tiles_of(g), channels(peer, first, count)],
            dst_ref=r1.at[l, me, tiles_of(g), pl.ds(first, count)],
            send_sem=a_send.at[l, slot, d - 1],
            recv_sem=a_recv.at[l, slot, d - 1],
            device_id={"lon": peer},
            device_id_type=MESH,
        )

    def b_copy(l, g, part, d):
        slot, first, count = part
        peer = lax.rem(me + d, LON)
        return pltpu.make_async_remote_copy(
            src_ref=s2.at[l, peer, tiles_of(g), pl.ds(first, count)],
            dst_ref=r2.at[l, tiles_of(g), channels(me, first, count)],
            send_sem=b_send.at[l, slot, d - 1],
            recv_sem=b_recv.at[l, slot, d - 1],
            device_id={"lon": peer},
            device_id_type=MESH,
        )

    def halo_copy(l, g):
        return pltpu.make_async_remote_copy(
            src_ref=xr.at[l, pl.ds(2 + 5 * g, 2)],
            dst_ref=xr.at[l, pl.ds(14 - 7 * g, 2)],
            send_sem=h_send.at[l, g // 2],
            recv_sem=h_recv.at[l, g // 2],
            device_id={"lat": lax.rem(lat + lats + g - 1, lats)},
            device_id_type=MESH,
        )

    def start_a(l, g, place):
        for part in A_PARTS[place]:
            for d in range(1, LON):
                a_copy(l, g, part, d).start()
        r1[l, me, tiles_of(g)] = xpos[l, tiles_of(g), mine]

    def pack_input(g):
        def piece(i):
            at = pl.ds(pl.multiple_of(i * 128, 128), 128)
            for third in range(3):
                lons = pl.ds(32 * third, 32)
                tile = jnp.concatenate([rows_in[4 * g + r, lons, at] for r in range(4)], axis=0)
                xpos[0, 3 * g + third, at, :] = tile.T

        loop(C // 128, piece)

    for place, g in enumerate((1, 0, 2)):
        fetch(g).wait()
        pack_input(g)
        if place == 0:
            pl.semaphore_wait(barrier, LON + 1)
        start_a(0, g, place)

    def unit_matrix(n):
        return (
            lax.broadcasted_iota(jnp.int32, (n, n), 0)
            == lax.broadcasted_iota(jnp.int32, (n, n), 1)
        ).astype(BF16)

    loads[0].wait()
    loads[1].wait()
    taps_basis = [unit_place((32 * u - TAPS // 2) % W // 32) for u in range(TAPS // 32)]

    def spectra(i):
        l = i // KROWS
        r = lax.rem(i, KROWS)
        pick = (
            lax.broadcasted_iota(jnp.int32, (SHARE, C), 1)
            == lax.broadcasted_iota(jnp.int32, (SHARE, C), 0) + me * SHARE
        ).astype(BF16)
        taps = nt(pick, kraw[l, r]).astype(BF16)
        tap_rows = jnp.concatenate([fb[p : p + 32, :] for p in taps_basis], axis=0)
        full = nn(taps, tap_rows)
        keep = lax.broadcasted_iota(jnp.int32, (SHARE, HALF), 1) >= 1
        scale = jnp.where(keep, 2.0 / W, 1.0 / W).astype(F32)
        real = full[:, :HALF] * scale
        sine = full[:, HALF:] * scale
        kf[l, r, 0] = real
        kf[l, r, 1] = jnp.where(keep, sine, 0.0)
        kf[l, r, 2] = jnp.where(keep, real, sine)

    loop(BLOCKS * KROWS, spectra)

    def turn0(i):
        at = pl.ds(pl.multiple_of(i * 256, 256), 256)
        fbt[at, :] = nt(unit_matrix(256), fb[:, at]).astype(BF16)

    loop(W // 256, turn0)
    loads[2].wait()
    loads[3].wait()

    for l in range(BLOCKS):

        def turn1(i):
            at = pl.ds(pl.multiple_of(i * 256, 256), 256)
            w1t[l, at, :] = nt(unit_matrix(256), w1[l, :, at]).astype(BF16)

        def turn2(i):
            at = pl.ds(pl.multiple_of(i * 128, 128), 128)
            w2t[l, at, :] = nt(unit_matrix(128), w2[l, :, at]).astype(BF16)
            row = jnp.broadcast_to(gain_ref[pl.ds(l, 1), at].astype(F32), (128, 128))
            gainb[l, at, :] = row.T

        loop(FF // 256, turn1)
        loop(C // 128, turn2)

    def unpack(l, g, first, count):
        some = pl.ds(first, count)

        def piece(third):
            for half in range(2):
                tiles = [r1[l, 4 * half + q, 3 * g + third, some, :] for q in range(4)]
                rows = swap4(tiles)
                at = pl.ds(pl.multiple_of(256 * third, 128) + 128 * half, 128)
                for r in range(4):
                    xr[l, 2 + 4 * g + r, some, at] = rows[r]

        loop(3, piece)

    def transform(l, top, rows, first, count):
        some = pl.ds(first, count)
        lhs = xr[l, pl.ds(top, rows), some, :].reshape(rows * count, W)
        for n in range(3):
            at = pl.ds(256 * n, 256)
            part = nn(lhs, fb[:, at])
            for r in range(rows):
                weight = quad_ref[lat * ROWS + top + r]
                spec[top + r, some, at] = part[count * r : count * (r + 1)] * weight

    def convolve(l, g, first, count):
        some = pl.ds(first, count)

        def bands(i):
            rows = pl.ds(pl.multiple_of(first + i * 16, 16), 16)
            for n in range(3):
                re_at = pl.ds(128 * n, 128)
                im_at = pl.ds(HALF + 128 * n, 128)
                factors = [
                    [kf[l, r, j, rows, re_at] for j in range(3)] for r in range(KROWS)
                ]
                for row in range(4):
                    real = sine = None
                    for r in range(KROWS):
                        a = spec[4 * g + row + r, rows, re_at]
                        b = spec[4 * g + row + r, rows, im_at]
                        kr, kc, ks = factors[r]
                        new_real = a * kr - b * kc
                        new_sine = a * kc + b * ks
                        real = new_real if real is None else real + new_real
                        sine = new_sine if sine is None else sine + new_sine
                    yb[row, rows, re_at] = real.astype(BF16)
                    yb[row, rows, im_at] = sine.astype(BF16)

        loop(count // 16, bands)

        lhs = yb[:, some, :].reshape(4 * count, W)
        for third in range(3):
            at = 256 * third
            part = nn(lhs, fbt[:, pl.ds(at, 256)])
            for half in range(2):
                tiles = []
                for r in range(4):
                    conv = part[count * r : count * (r + 1), 128 * half : 128 * (half + 1)]
                    old = xr[l, 2 + 4 * g + r, some, pl.ds(at + 128 * half, 128)]
                    tiles.append((old.astype(F32) + gelu(conv)).astype(BF16))
                packed = swap4(tiles)
                for q in range(4):
                    s2[l, 4 * half + q, 3 * g + third, some, :] = packed[q]

    def start_b(l, g, part):
        slot, first, count = part
        for d in range(1, LON):
            b_copy(l, g, part, d).start()
        r2[l, tiles_of(g), channels(me, first, count)] = s2[
            l, me, tiles_of(g), pl.ds(first, count)
        ]

    def feed_forward(l, g):
        def norm(t):
            values = r2[l, 3 * g + t].astype(F32)
            average = jnp.sum(values, axis=0, keepdims=True) * (1.0 / C)
            centred = values - average
            variance = jnp.sum(centred * centred, axis=0, keepdims=True) * (1.0 / C)
            scaled = centred * lax.rsqrt(variance + 1e-05) * gainb[l]
            nrm[:, pl.ds(pl.multiple_of(128 * t, 128), 128)] = scaled.astype(BF16)

        loop(3, norm)

        for i in range(FF // 256):
            at = pl.ds(i * 256, 256)
            hid[at, :] = gelu(nn(w1t[l, at, :], nrm[...])).astype(BF16)
        out = nn(w2t[l], hid[...])
        for t in range(3):
            old = r2[l, 3 * g + t].astype(F32)
            new = (old + out[:, 128 * t : 128 * (t + 1)]).astype(BF16)
            xpos[1 - l, 3 * g + t] = new

    def finish(g):
        def piece(i):
            at = pl.ds(pl.multiple_of(i * 128, 128), 128)
            for third in range(3):
                turned = xpos[0, 3 * g + third, at, :].T
                for r in range(4):
                    out_ref[0, 4 * g + r, pl.ds(32 * third, 32), at] = turned[
                        32 * r : 32 * (r + 1), :
                    ]

        loop(C // 128, piece)

    def take(l, g, part, rim=False):
        for d in range(1, LON):
            a_copy(l, g, part, d).wait_recv()
        unpack(l, g, *part[1:])
        if rim:
            halo_copy(l, g).start()
        transform(l, 2 + 4 * g, 4, *part[1:])

    def give(l, g, part):
        convolve(l, g, *part[1:])
        start_b(l, g, part)

    def block(l):
        early, late = 2 * l, 2 - 2 * l
        take(l, 1, A_PARTS[0][0])
        take(l, early, A_PARTS[1][0], rim=True)
        for place, (arrived, ready) in enumerate(zip(A_PARTS[2], B_PARTS[0])):
            take(l, late, arrived, rim=place == 1)
            give(l, 1, ready)
        for place, g in ((1, late), (2, early)):
            halo_copy(l, 2 - g).wait_recv()
            transform(l, 7 * g, 2, 0, SHARE)
            give(l, g, B_PARTS[place][0])
        for place, g in enumerate((1, late, early)):
            for part in B_PARTS[place]:
                for d in range(1, LON):
                    b_copy(l, g, part, d).wait_recv()
            feed_forward(l, g)

            @pl.when(l == 0)
            def _():
                start_a(1, g, place)

            @pl.when(l == BLOCKS - 1)
            def _():
                finish(g)

        for a_place, g in enumerate((1, early, late)):
            for d in range(1, LON):
                for part in A_PARTS[a_place]:
                    a_copy(l, g, part, d).wait_send()
        for b_place, g in enumerate((1, late, early)):
            for d in range(1, LON):
                for part in B_PARTS[b_place]:
                    b_copy(l, g, part, d).wait_send()
        halo_copy(l, early).wait_send()
        halo_copy(l, late).wait_send()

    loop(BLOCKS, block)


def body(ocean_state, zonal_kernel, norm_gain, input_weight, output_weight):
    total = ROWS * lax.axis_size("lat")
    quad = jnp.asarray(row_weights(total))
    table = jnp.asarray(basis().astype(jnp.bfloat16))
    state = jnp.transpose(ocean_state, (0, 1, 3, 2))
    hbm = pl.BlockSpec(memory_space=pl.ANY)
    out = pl.pallas_call(
        kernel,
        out_shape=pltpu.VMEM((1, ROWS, COLS, C), BF16),
        in_specs=[
            pl.BlockSpec(memory_space=pltpu.SMEM),
            pl.BlockSpec(memory_space=pltpu.VMEM),
            hbm, hbm, hbm, hbm, hbm,
        ],
        out_specs=pl.BlockSpec(memory_space=pltpu.VMEM),
        scratch_shapes=[
            pltpu.VMEM((ROWS, COLS, C), BF16),
            pltpu.VMEM((2, TILES, C, 128), BF16),
            pltpu.VMEM((2, LON, TILES, SHARE, 128), BF16),
            pltpu.VMEM((2, ROWS + 4, SHARE, W), BF16),
            pltpu.VMEM((ROWS + 4, SHARE, W), F32),
            pltpu.VMEM((2, KROWS, 3, SHARE, HALF), F32),
            pltpu.VMEM((4, SHARE, W), BF16),
            pltpu.VMEM((2, LON, TILES, SHARE, 128), BF16),
            pltpu.VMEM((2, TILES, C, 128), BF16),
            pltpu.VMEM((2, FF, C), BF16),
            pltpu.VMEM((2, C, FF), BF16),
            pltpu.VMEM((FF, 384), BF16),
            pltpu.VMEM((C, 384), BF16),
            pltpu.VMEM((2, C, 128), F32),
            pltpu.VMEM((W, W), BF16),
            pltpu.VMEM((W, W), BF16),
            pltpu.VMEM((BLOCKS, KROWS, TAPS, C), BF16),
            pltpu.VMEM((BLOCKS, C, FF), BF16),
            pltpu.VMEM((BLOCKS, FF, C), BF16),
            pltpu.SemaphoreType.DMA((GROUPS,)),
            pltpu.SemaphoreType.DMA((4,)),
            pltpu.SemaphoreType.DMA((2, GROUPS + 1, LON - 1)),
            pltpu.SemaphoreType.DMA((2, GROUPS + 1, LON - 1)),
            pltpu.SemaphoreType.DMA((2, GROUPS + 1, LON - 1)),
            pltpu.SemaphoreType.DMA((2, GROUPS + 1, LON - 1)),
            pltpu.SemaphoreType.DMA((2, 2)),
            pltpu.SemaphoreType.DMA((2, 2)),
        ],
        compiler_params=pltpu.CompilerParams(
            collective_id=0, has_side_effects=True, vmem_limit_bytes=54 * 1024 * 1024
        ),
    )(quad, norm_gain, state, zonal_kernel, input_weight, output_weight, table)
    return jnp.transpose(out, (0, 1, 3, 2))


def solution(mesh):
    in_specs = (P(None, "lat", None, "lon"), P(), P(), P(), P())
    out_specs = P(None, "lat", None, "lon")
    return jax.shard_map(body, mesh=mesh, in_specs=in_specs, out_specs=out_specs, check_vma=False)
```
